1024 devices in a mesh: dp: 16 (over x_lo, y, core), tensor: 64 (over x_hi, z).
Axes of the slice: x: 4 (x_hi: 2, x_lo: 2; x = x_hi * 2 + x_lo), y: 4, z: 32, core: 2. Of those that a mesh axis runs over, the one named last changes fastest.
Arguments:
- query_latent: bfloat16 [2048, 1536], P(('dp', 'tensor')), may hold values from -40 to 40
- key_value_latent: bfloat16 [2048, 512], P(('dp', 'tensor')), may hold values from -40 to 40
- query_gain: float32 [1536], replicated, may hold values from 0.5 to 1.5
- key_value_gain: float32 [512], replicated, may hold values from 0.5 to 1.5
- q_up: bfloat16 [1536, 24576], P(None, 'tensor'), may hold values from -0.625 to 0.625
- kv_up: bfloat16 [512, 32768], P(None, 'tensor'), may hold values from -1 to 1
- grad_q: bfloat16 [2048, 24576], P('dp', 'tensor'), may hold values from -0.23925781 to 0.23925781
- grad_kv: bfloat16 [2048, 32768], P('dp', 'tensor'), may hold values from -0.23925781 to 0.23925781
Outputs:
- query_latent_gradient: float32 [2048, 1536], P(('dp', 'tensor'))
- key_value_latent_gradient: float32 [2048, 512], P(('dp', 'tensor'))
- d_q_up: float32 [1536, 24576], P('dp', 'tensor')
- d_kv_up: float32 [512, 32768], P('dp', 'tensor')
The draws below stay inside these ranges and needn't reach their ends.
All inputs are finite; a program needn't handle non-finite values.
Results may differ from the reference program's by a relative error of at most 0.0029.
Values may be sent and summed in bfloat16 or wider, within the bound.
A program may use at most 32 MiB of HBM per device.

```python
import math
import jax
import jax.numpy as jnp
from jax import lax

QL = 1536
KVL = 512
NOPE = 128
ROPE = 64
VDIM = 128
HEADS = 128
TOK_ALL = 2048
N_DP = 16


def scaled_latent(key, rows, cols):
    key_rows, key_cols, key_base = jax.random.split(key, 3)
    row_scale = 0.3 * jnp.exp(jax.random.uniform(key_rows, (rows, 1), minval=0.0, maxval=math.log(10.0)))
    col_scale = 0.3 * jnp.exp(jax.random.uniform(key_cols, (1, cols), minval=0.0, maxval=math.log(10.0)))
    base = jax.random.normal(key_base, (rows, cols))
    input_values = jnp.clip(base * row_scale * col_scale, -40.0, 40.0)
    return input_values.astype(jnp.bfloat16)


def draw_query_latent(key, part):
    return scaled_latent(jax.random.fold_in(key, 11), TOK_ALL, QL)


def draw_key_value_latent(key, part):
    return scaled_latent(jax.random.fold_in(key, 23), TOK_ALL, KVL)


def steps_of(own_key, extent, cuts, low, high):
    def one(dim, shards_of):
        heights = jax.random.uniform(jax.random.fold_in(jax.random.fold_in(own_key, 6), dim), (shards_of,), jnp.float32, low / len(cuts), high / len(cuts))
        return jnp.repeat(jnp.exp(heights), extent[dim] // shards_of).reshape((-1,) + (1,) * (len(extent) - dim - 1))

    factor_of = one(*cuts[0])
    for cut in cuts[1:]:
        factor_of = factor_of * one(*cut)
    return factor_of


def centred(key, shape, scale, bound, cuts=(), held_as=jnp.bfloat16):
    drawn = jax.random.normal(key, shape, jnp.float32) * scale
    if len(cuts) > 0:
        drawn = steps_of(key, shape, cuts, -0.22, 0.18) * drawn
    return jnp.clip(drawn, min=-bound, max=bound).astype(held_as)


def setup_inputs(seed: int = 0) -> dict:
    streams_of = jax.random.split(jax.random.key(seed), 9)
    query_latent = draw_query_latent(jax.random.fold_in(streams_of[8], 71), 0)
    key_value_latent = draw_key_value_latent(jax.random.fold_in(streams_of[8], 71), 0)
    query_gain = jnp.clip(1.0 + 0.1 * jax.random.normal(streams_of[2], (QL,), jnp.float32), 0.5, 1.5)
    key_value_gain = jnp.clip(1.0 + 0.1 * jax.random.normal(streams_of[3], (KVL,), jnp.float32), 0.5, 1.5)
    q_up = centred(streams_of[4], (QL, HEADS * (NOPE + ROPE)), (QL // 16) ** -0.5, 0.625, ((1, 64),))
    kv_up = centred(streams_of[5], (KVL, HEADS * (NOPE + VDIM)), (KVL // 16) ** -0.5, 1.0, ((1, 64),))
    grad_q = centred(streams_of[6], (TOK_ALL, HEADS * (NOPE + ROPE)), 0.04, 0.23925781, ((0, 16), (1, 64)))
    grad_kv = centred(streams_of[7], (TOK_ALL, HEADS * (NOPE + VDIM)), 0.04, 0.23925781, ((0, 16), (1, 64)))
    return {"query_latent": query_latent, "key_value_latent": key_value_latent, "query_gain": query_gain, "key_value_gain": key_value_gain, "q_up": q_up, "kv_up": kv_up, "grad_q": grad_q, "grad_kv": grad_kv}


EPS = 1e-06

def apply_norm(raw, norm_gain):
    input_values = raw.astype(jnp.float32)
    inverse_norm = lax.rsqrt(lax.optimization_barrier(jnp.mean(input_values * input_values, axis=-1, keepdims=True)) + EPS)
    unit_input = input_values * inverse_norm
    return (unit_input, inverse_norm, (norm_gain * unit_input).astype(jnp.bfloat16))

def backward_of_norm(incoming_gradient, unit_input, inverse_norm, norm_gain):
    scaled_gradient = norm_gain * incoming_gradient
    mean_correction = lax.optimization_barrier(jnp.mean(scaled_gradient * unit_input, axis=-1, keepdims=True))
    return inverse_norm * (scaled_gradient - unit_input * mean_correction)

def group_weights(normed, cotangent):
    groups = normed.reshape(N_DP, -1, normed.shape[1])
    cot_groups = cotangent.reshape(N_DP, -1, cotangent.shape[1])

    def step(total, pair):
        part = lax.dot_general(pair[0], pair[1], (((0,), (0,)), ((), ())), preferred_element_type=jnp.float32)
        return (total + part, None)
    start = jnp.zeros((normed.shape[1], cotangent.shape[1]), jnp.float32)
    total, unused_item = lax.scan(step, start, (groups, cot_groups))
    return total

def reference(query_latent, key_value_latent, query_gain, key_value_gain, q_up, kv_up, grad_q, grad_kv):
    query_unit, query_inverse_norm, query_normed = apply_norm(query_latent, query_gain)
    key_value_unit, key_value_inverse_norm, key_value_normed = apply_norm(key_value_latent, key_value_gain)
    d_q_up = group_weights(query_normed, grad_q)
    d_kv_up = group_weights(key_value_normed, grad_kv)
    query_norm_gain = lax.dot_general(grad_q, q_up, (((1,), (1,)), ((), ())), preferred_element_type=jnp.float32)
    key_value_norm_gain = lax.dot_general(grad_kv, kv_up, (((1,), (1,)), ((), ())), preferred_element_type=jnp.float32)
    query_latent_gradient = backward_of_norm(query_norm_gain, query_unit, query_inverse_norm, query_gain)
    key_value_latent_gradient = backward_of_norm(key_value_norm_gain, key_value_unit, key_value_inverse_norm, key_value_gain)
    return (query_latent_gradient, key_value_latent_gradient, d_q_up, d_kv_up)
```

```python
import jax
import jax.numpy as jnp
from jax import lax
from jax.experimental import pallas as pl
from jax.experimental.pallas import tpu as pltpu
from jax.sharding import PartitionSpec as P

MESH = pl.DeviceIdType.MESH
F32 = jnp.float32
BF16 = jnp.bfloat16
EPS = 1e-06

NEAR = [(1, 0), (2, 0), (3, 0), (0, 1), (1, 1), (2, 1), (3, 1)]
FAR = [1, 7, 2, 6, 3, 5, 4]
PLANE = [(0, 0), (1, 0), (0, 3), (0, 1), (1, 3), (1, 1), (0, 2), (1, 2)]


def iota(shape, dim):
    return lax.broadcasted_iota(jnp.int32, shape, dim)


def one_hot(mask):
    return jnp.where(mask, 1.0, 0.0).astype(BF16)


def dot(a, b, dims):
    return lax.dot_general(a, b, (dims, ((), ())), preferred_element_type=F32)


def kernel(
    ql_hbm, kvl_hbm, qg_hbm, kvg_hbm, qup_hbm, kvup_hbm, gq_hbm, gkv_hbm,
    dql_ref, dkvl_ref, dqup_ref, dkvup_ref,
    ql, kvl, qg, kvg, qup, kvup, grads,
    pack, mixed, piece, gall, xall, part, near_in, send_far, far_in, natural, acc,
    load_sem, mix_send, mix_recv, plane_send, plane_recv, pair_send, pair_recv,
    rnear_send, rnear_recv, rfar_send, rfar_recv, afar_send, afar_recv, anear_send, anear_recv,
    ready,
):
    dp, tensor = lax.axis_index("dp"), lax.axis_index("tensor")
    c = lax.rem(dp, 2)
    y = lax.rem(dp // 2, 4)
    xl = dp // 8
    z = lax.rem(tensor, 32)
    xh = tensor // 32
    r = lax.rem(z, 4)
    j = z // 4
    width = 4 * c - 2
    steps = [0, 1, -1, width]

    def along(dz, flip=0):
        half = 1 - xh if flip else xh
        return (dp, half * 32 + lax.rem(z + dz + 32, 32))

    def chip(dx, dy, other=0):
        px = 1 - xl if dx else xl
        core = 1 - c if other else c
        return (px * 4 + lax.rem(y + dy, 4)) * 2 + core

    barrier = pltpu.get_barrier_semaphore()
    peers = [(lax.rem(dp + k, 16), tensor) for k in range(1, 16)]
    peers += [along(dz, flip) for flip in (0, 1) for dz in (1, -1, 2, -2)]
    peers += [along(0, 1), along(4), along(-4)]
    for peer in peers:
        pl.semaphore_signal(barrier, inc=1, device_id=peer, device_id_type=MESH)

    loads = [
        pltpu.make_async_copy(src, dst, load_sem.at[n])
        for n, (src, dst) in enumerate([
            (ql_hbm, ql), (kvl_hbm, kvl), (qg_hbm, qg), (kvg_hbm, kvg),
            (gq_hbm, grads.at[:, 0:384]), (gkv_hbm, grads.at[:, 384:896]),
            (qup_hbm, qup), (kvup_hbm, kvup),
        ])
    ]
    for load in loads:
        load.start()
    sent = []

    def send(src, dst, send_sem, recv_sem, device):
        copy = pltpu.make_async_remote_copy(
            src_ref=src, dst_ref=dst, send_sem=send_sem, recv_sem=recv_sem,
            device_id=device, device_id_type=MESH)
        copy.start()
        return copy

    for load in loads[:4]:
        load.wait()

    def norm(raw, gain):
        wide = raw[...].astype(F32)
        inverse = lax.rsqrt(jnp.mean(wide * wide, axis=-1, keepdims=True) + EPS)
        unit = wide * inverse
        return unit, inverse, gain[...] * unit

    q_unit, q_inv, q_normed = norm(ql, qg)
    kv_unit, kv_inv, kv_normed = norm(kvl, kvg)
    for b in range(16):
        pack[b, :, 0:96] = q_normed[:, 96 * b : 96 * b + 96]
        pack[b, :, 96:128] = kv_normed[:, 32 * b : 32 * b + 32]

    for load in loads[4:6]:
        load.wait()
    row, col = iota((128, 128), 0), iota((128, 128), 1)
    token = ((row >> 4) & 1) * 64 + ((row >> 1) & 7) * 8 + (row >> 5) * 2 + (row & 1)
    order = one_hot(col == token)
    ordered = dot(order, grads[...], ((1,), (0,))).astype(BF16)
    gall[dp] = ordered.reshape(4, 2, 16, 896)
    mixed[dp] = pack[dp]

    pl.semaphore_wait(barrier, len(peers))
    pl.semaphore_signal(ready.at[0], inc=1, device_id=along(-4), device_id_type=MESH)
    pl.semaphore_signal(ready.at[1], inc=1, device_id=along(4), device_id_type=MESH)

    mixes = []
    for k in range(1, 16):
        to = lax.rem(dp + k, 16)
        mixes.append(send(pack.at[to], mixed.at[dp], mix_send.at[k], mix_recv.at[k], (to, tensor)))

    def relay(n, dx, dy):
        return gall.at[chip(*PLANE[n])]

    def pass_on(n, slot, dx, dy):
        at = gall.at[chip(*PLANE[n])]
        return send(at, at, plane_send.at[slot], plane_recv.at[slot], (chip(dx, dy), tensor))

    def to_pair(n):
        at = gall.at[chip(*PLANE[n])]
        return send(at, at, pair_send.at[n], pair_recv.at[n], (chip(0, 0, 1), tensor))

    plane = {}
    plane[1] = pass_on(0, 1, 1, 0)
    plane[2] = pass_on(0, 2, 0, 1)
    plane[3] = pass_on(0, 3, 0, 3)
    pairs = [to_pair(0)]

    loads[6].wait()
    loads[7].wait()
    own = gall[dp].reshape(128, 896)
    for q in range(4):
        if q < 3:
            value = dot(own[:, 0:384], qup[512 * q : 512 * q + 512, :], ((1,), (1,)))
        else:
            value = dot(own[:, 384:896], kvup[...], ((1,), (1,)))
        part[:, :, q] = value.astype(BF16).reshape(4, 2, 16, 512)

    rnear = []
    for n, (s, flip) in enumerate(NEAR):
        device = along(steps[s], flip)
        half = 1 - xh if flip else xh
        cls = lax.rem(z + steps[s] + 32, 4)
        rnear.append(send(part.at[cls, half], near_in.at[n], rnear_send.at[n], rnear_recv.at[n], device))

    pl.semaphore_wait(ready.at[0], 1)
    pl.semaphore_wait(ready.at[1], 1)
    pl.semaphore_signal(ready.at[2], inc=1, device_id=along(-8), device_id_type=MESH)
    pl.semaphore_signal(ready.at[3], inc=1, device_id=along(8), device_id_type=MESH)

    for copy in mixes:
        copy.wait_recv()
    for b in range(16):
        piece[2 * b : 2 * b + 2, :] = mixed[b]
    xall[xh, r, j] = piece[...].astype(BF16)

    def far_send(k):
        at = xall.at[xh, r, j]
        return send(at, at, afar_send.at[k], afar_recv.at[k], along(4 * k))

    def near_forward(k):
        at = xall.at[xh, r, lax.rem(j + 8 - k, 8)]
        for n, (s, flip) in enumerate(NEAR):
            send(at, at, anear_send.at[n], anear_recv.at[n], along(steps[s], flip))

    afar = {}
    for k in FAR[:4]:
        afar[k] = far_send(k)
    near_forward(0)
    pl.semaphore_wait(ready.at[2], 1)
    pl.semaphore_wait(ready.at[3], 1)
    for k in FAR[4:]:
        afar[k] = far_send(k)

    plane[1].wait_recv()
    plane[4] = pass_on(1, 4, 0, 1)
    plane[5] = pass_on(1, 5, 0, 3)
    pairs.append(to_pair(1))
    plane[2].wait_recv()
    plane[6] = pass_on(2, 6, 0, 1)
    pairs.append(to_pair(2))
    plane[3].wait_recv()
    pairs.append(to_pair(3))

    for k in FAR[:2]:
        afar[k].wait_recv()
        near_forward(k)

    for copy in rnear:
        copy.wait_recv()
    total = part[r, xh].astype(F32)
    for n in range(7):
        total = total + near_in[n].astype(F32)
    row, col = iota((64, 64), 0), iota((64, 64), 1)
    spread = one_hot(col == (row & 3) * 16 + (row >> 3) * 2 + ((row >> 2) & 1))
    total = dot(spread, total.astype(BF16).reshape(64, 512), ((1,), (0,)))
    send_far[...] = total.astype(BF16).reshape(8, 8, 512)

    for k in FAR[2:4]:
        afar[k].wait_recv()
        near_forward(k)

    rfar = []
    for k in FAR:
        rfar.append(send(send_far.at[lax.rem(j + k, 8)], far_in.at[k], rfar_send.at[k], rfar_recv.at[k], along(4 * k)))

    plane[4].wait_recv()
    pairs.append(to_pair(4))
    plane[5].wait_recv()
    plane[7] = pass_on(5, 7, 0, 3)
    pairs.append(to_pair(5))
    plane[6].wait_recv()
    pairs.append(to_pair(6))

    for k in FAR[4:]:
        afar[k].wait_recv()
        near_forward(k)
    plane[7].wait_recv()
    pairs.append(to_pair(7))
    for copy in pairs:
        copy.wait_recv()

    row, col = iota((256, 256), 0), iota((256, 256), 1)
    regroup = one_hot(col == ((row >> 1) & 15) * 16 + (row >> 5) * 2 + (row & 1))

    def weights(half, cls):
        x = dot(xall[half, cls].reshape(256, 128), regroup, ((0,), (0,))).astype(BF16)
        g = gall[:, cls, half].reshape(256, 896)
        return dot(x, g, ((1,), (0,)))

    acc[...] = weights(xh, r)

    for copy in rfar:
        copy.wait_recv()
    latent = send_far[j].astype(F32)
    for k in range(1, 8):
        latent = latent + far_in[k].astype(F32)
    for i in range(2):
        for q in range(4):
            natural[i : i + 1, 512 * q : 512 * q + 512] = latent[4 * i + q : 4 * i + q + 1, :]

    def norm_back(incoming, unit, inverse, gain):
        scaled = gain[...] * incoming
        mean = jnp.mean(scaled * unit, axis=-1, keepdims=True)
        return inverse * (scaled - unit * mean)

    q_unit, q_inv, q_normed = norm(ql, qg)
    kv_unit, kv_inv, kv_normed = norm(kvl, kvg)
    dql_ref[...] = norm_back(natural[:, 0:1536], q_unit, q_inv, qg)
    dkvl_ref[...] = norm_back(natural[:, 1536:2048], kv_unit, kv_inv, kvg)

    for n, (s, flip) in enumerate(NEAR):
        half = 1 - xh if flip else xh
        cls = lax.rem(z - steps[s] + 32, 4)
        whole = xall.at[half, cls]
        pltpu.make_async_remote_copy(
            src_ref=whole, dst_ref=whole, send_sem=anear_send.at[n], recv_sem=anear_recv.at[n],
            device_id=along(steps[s], flip), device_id_type=MESH).wait_recv()
        acc[...] += weights(half, cls)
    dqup_ref[...] = acc[0:96, 0:384]
    dkvup_ref[...] = acc[96:128, 384:896]

    for copy in mixes + list(plane.values()) + pairs + rnear + rfar + list(afar.values()):
        copy.wait_send()
    for n, (s, flip) in enumerate(NEAR):
        whole = xall.at[xh, r]
        pltpu.make_async_remote_copy(
            src_ref=whole, dst_ref=whole, send_sem=anear_send.at[n], recv_sem=anear_recv.at[n],
            device_id=along(steps[s], flip), device_id_type=MESH).wait_send()


def body(query_latent, key_value_latent, query_gain, key_value_gain, q_up, kv_up, grad_q, grad_kv):
    dma = pltpu.SemaphoreType.DMA
    vmem = pltpu.VMEM
    return pl.pallas_call(
        kernel,
        name="mla_up_backward",
        out_shape=(
            jax.ShapeDtypeStruct((2, 1536), F32),
            jax.ShapeDtypeStruct((2, 512), F32),
            jax.ShapeDtypeStruct((96, 384), F32),
            jax.ShapeDtypeStruct((32, 512), F32),
        ),
        in_specs=[pl.BlockSpec(memory_space=pltpu.HBM)] * 8,
        out_specs=(pl.BlockSpec(memory_space=pltpu.VMEM),) * 4,
        scratch_shapes=[
            vmem((2, 1536), BF16), vmem((2, 512), BF16), vmem((1, 1536), F32), vmem((1, 512), F32),
            vmem((1536, 384), BF16), vmem((512, 512), BF16), vmem((128, 896), BF16),
            vmem((16, 2, 128), F32),
            vmem((16, 2, 128), F32),
            vmem((32, 128), F32),
            vmem((16, 4, 2, 16, 896), BF16),
            vmem((2, 4, 8, 32, 128), BF16),
            vmem((4, 2, 4, 16, 512), BF16),
            vmem((7, 4, 16, 512), BF16),
            vmem((8, 8, 512), BF16),
            vmem((8, 8, 512), BF16),
            vmem((2, 2048), F32),
            vmem((128, 896), F32),
            dma((8,)), dma((16,)), dma((16,)), dma((8,)), dma((8,)), dma((8,)), dma((8,)),
            dma((7,)), dma((7,)), dma((8,)), dma((8,)), dma((8,)), dma((8,)), dma((7,)), dma((7,)),
            pltpu.SemaphoreType.REGULAR((4,)),
        ],
        compiler_params=pltpu.CompilerParams(
            collective_id=0, has_side_effects=True, vmem_limit_bytes=48 * 1024 * 1024),
    )(query_latent, key_value_latent, query_gain.reshape(1, -1), key_value_gain.reshape(1, -1), q_up, kv_up, grad_q, grad_kv)


def solution(mesh):
    group = ("dp", "tensor")
    placed = (
        P(group, None), P(group, None), P(), P(), P(None, "tensor"), P(None, "tensor"),
        P("dp", "tensor"), P("dp", "tensor"),
    )
    return jax.shard_map(
        body,
        mesh=mesh,
        in_specs=placed,
        out_specs=(P(group, None), P(group, None), P("dp", "tensor"), P("dp", "tensor")),
        check_vma=False,
    )
```

```python
import jax
import jax.numpy as jnp
from jax import lax
from jax.experimental import pallas as pl
from jax.experimental.pallas import tpu as pltpu
from jax.sharding import PartitionSpec as P

MESH = pl.DeviceIdType.MESH
F32 = jnp.float32
BF16 = jnp.bfloat16
EPS = 1e-06
scope = jax.named_scope

NEAR = [(1, 0), (2, 0), (3, 0), (0, 1), (1, 1), (2, 1), (3, 1)]
FAR = [1, 7, 2, 6, 3, 5, 4]
PLANE = [(0, 0), (1, 0), (0, 3), (0, 1), (1, 3), (1, 1), (0, 2), (1, 2)]


def iota(shape, dim):
    return lax.broadcasted_iota(jnp.int32, shape, dim)


def one_hot(mask):
    return jnp.where(mask, 1.0, 0.0).astype(BF16)


def dot(a, b, dims):
    return lax.dot_general(a, b, (dims, ((), ())), preferred_element_type=F32)


def kernel(
    ql_hbm, kvl_hbm, qg_hbm, kvg_hbm, qup_hbm, kvup_hbm, gq_hbm, gkv_hbm,
    dql_hbm, dkvl_hbm, dqup_hbm, dkvup_hbm,
    ql, kvl, qg, kvg, qup, kvup, grads,
    pack, mixed, piece, gall, xall, part, near_in, send_far, far_in, natural, acc,
    load_sem, mix_send, mix_recv, plane_send, plane_recv, pair_send, pair_recv,
    rnear_send, rnear_recv, rfar_send, rfar_recv, afar_send, afar_recv, anear_send, anear_recv,
    dql, dkvl, out_sem, ready,
):
    dp, tensor = lax.axis_index("dp"), lax.axis_index("tensor")
    c = lax.rem(dp, 2)
    y = lax.rem(dp // 2, 4)
    xl = dp // 8
    z = lax.rem(tensor, 32)
    xh = tensor // 32
    r = lax.rem(z, 4)
    j = z // 4
    width = 4 * c - 2
    steps = [0, 1, -1, width]

    def along(dz, flip=0):
        half = 1 - xh if flip else xh
        return (dp, half * 32 + lax.rem(z + dz + 32, 32))

    def chip(dx, dy, other=0):
        px = 1 - xl if dx else xl
        core = 1 - c if other else c
        return (px * 4 + lax.rem(y + dy, 4)) * 2 + core

    barrier = pltpu.get_barrier_semaphore()
    peers = [along(4), along(-4)]
    peers += [along(dz, flip) for flip in (1, 0) for dz in (2, -2, 1, -1)]
    peers += [(lax.rem(dp + k, 16), tensor) for k in range(15, 0, -1)]
    peers += [along(0, 1)]
    for peer in peers:
        pl.semaphore_signal(barrier, inc=1, device_id=peer, device_id_type=MESH)

    loads = [
        pltpu.make_async_copy(src, dst, load_sem.at[n])
        for n, (src, dst) in enumerate([
            (ql_hbm, ql), (kvl_hbm, kvl), (qg_hbm, qg), (kvg_hbm, kvg),
            (gq_hbm, grads.at[:, 0:384]), (gkv_hbm, grads.at[:, 384:896]),
            (qup_hbm, qup), (kvup_hbm, kvup),
        ])
    ]
    for load in loads:
        load.start()
    sent = []

    def send(src, dst, send_sem, recv_sem, device):
        copy = pltpu.make_async_remote_copy(
            src_ref=src, dst_ref=dst, send_sem=send_sem, recv_sem=recv_sem,
            device_id=device, device_id_type=MESH)
        copy.start()
        return copy

    with scope("w_loadsmall"):
        for load in loads[:4]:
            load.wait()

    def norm(raw, gain):
        wide = raw[...].astype(F32)
        inverse = lax.rsqrt(jnp.mean(wide * wide, axis=-1, keepdims=True) + EPS)
        unit = wide * inverse
        return unit, inverse, gain[...].reshape(1, -1) * unit

    q_unit, q_inv, q_normed = norm(ql, qg)
    kv_unit, kv_inv, kv_normed = norm(kvl, kvg)
    for b in range(16):
        pack[b, :, 0:96] = q_normed[:, 96 * b : 96 * b + 96]
        pack[b, :, 96:128] = kv_normed[:, 32 * b : 32 * b + 32]

    with scope("w_loadgrads"):
        for load in loads[4:6]:
            load.wait()
    row, col = iota((128, 128), 0), iota((128, 128), 1)
    token = ((row >> 4) & 1) * 64 + ((row >> 1) & 7) * 8 + (row >> 5) * 2 + (row & 1)
    order = one_hot(col == token)
    ordered = dot(order, grads[...], ((1,), (0,))).astype(BF16)
    gall[dp] = ordered.reshape(4, 2, 16, 896)
    mixed[dp] = pack[dp]

    with scope("w_loadup"):
        loads[6].wait()
        loads[7].wait()
    own = gall[dp].reshape(128, 896)
    for q in range(4):
        if q < 3:
            value = dot(own[:, 0:384], qup[512 * q : 512 * q + 512, :], ((1,), (1,)))
        else:
            value = dot(own[:, 384:896], kvup[...], ((1,), (1,)))
        part[:, :, q] = value.astype(BF16).reshape(4, 2, 16, 512)

    with scope("w_barrier"):
        pl.semaphore_wait(barrier, len(peers))
    pl.semaphore_signal(ready.at[0], inc=1, device_id=along(-4), device_id_type=MESH)
    pl.semaphore_signal(ready.at[1], inc=1, device_id=along(4), device_id_type=MESH)

    mixes = []
    for k in range(1, 16):
        to = lax.rem(dp + k, 16)
        mixes.append(send(pack.at[to], mixed.at[dp], mix_send.at[k], mix_recv.at[k], (to, tensor)))

    whole, low, high = pl.ds(0, 4), pl.ds(0, 2), pl.ds(2, 2)

    def pass_on(n, slot, dx, dy, rows=whole):
        at = gall.at[chip(*PLANE[n]), rows]
        return send(at, at, plane_send.at[slot], plane_recv.at[slot], (chip(dx, dy), tensor))

    def to_pair(n, slot, rows=whole):
        at = gall.at[chip(*PLANE[n]), rows]
        return send(at, at, pair_send.at[slot], pair_recv.at[slot], (chip(0, 0, 1), tensor))

    rnear = []
    for n, (s, flip) in enumerate(NEAR):
        device = along(steps[s], flip)
        half = 1 - xh if flip else xh
        cls = lax.rem(z + steps[s] + 32, 4)
        rnear.append(send(part.at[cls, half], near_in.at[n], rnear_send.at[n], rnear_recv.at[n], device))

    plane = {}
    plane[2] = pass_on(0, 2, 0, 1)
    plane[3] = pass_on(0, 3, 0, 3)
    plane[1] = pass_on(0, 1, 1, 0)
    pairs = [to_pair(0, 0)]

    with scope("w_ready01"):
        pl.semaphore_wait(ready.at[0], 1)
        pl.semaphore_wait(ready.at[1], 1)
    pl.semaphore_signal(ready.at[2], inc=1, device_id=along(-8), device_id_type=MESH)
    pl.semaphore_signal(ready.at[3], inc=1, device_id=along(8), device_id_type=MESH)

    with scope("w_mixes"):
        for copy in mixes:
            copy.wait_recv()
    for b in range(16):
        piece[2 * b : 2 * b + 2, :] = mixed[b]
    xall[xh, r, j] = piece[...].astype(BF16)

    def far_pass(k, slot, dz):
        at = xall.at[xh, r, lax.rem(j + 8 - k, 8)]
        return send(at, at, afar_send.at[slot], afar_recv.at[slot], along(dz))

    def near_forward(k):
        at = xall.at[xh, r, lax.rem(j + 8 - k, 8)]
        for n, (s, flip) in enumerate(NEAR):
            send(at, at, anear_send.at[n], anear_recv.at[n], along(steps[s], flip))

    afar = {}
    afar[2] = far_pass(0, 2, 8)
    afar[6] = far_pass(0, 6, -8)
    afar[1] = far_pass(0, 1, 4)
    afar[7] = far_pass(0, 7, -4)
    near_forward(0)

    def await_plane(*slots):
        for slot in slots:
            with scope(f"w_plane{slot}"):
                plane[slot].wait_recv()

    def await_far(*slots):
        for slot in slots:
            with scope(f"w_afar{slot}"):
                afar[slot].wait_recv()

    await_plane(2)
    plane[6] = pass_on(2, 6, 0, 1, low)
    pairs.append(to_pair(2, 2))
    await_plane(3)
    plane[8] = pass_on(3, 8, 0, 3, high)
    pairs.append(to_pair(3, 3))
    for n, copy in enumerate(rnear):
        with scope(f"w_rnear{n}"):
            copy.wait_recv()
    total = part[r, xh].astype(F32)
    for n in range(7):
        total = total + near_in[n].astype(F32)
    row, col = iota((64, 64), 0), iota((64, 64), 1)
    spread = one_hot(col == (row & 3) * 16 + (row >> 3) * 2 + ((row >> 2) & 1))
    total = dot(spread, total.astype(BF16).reshape(64, 512), ((1,), (0,)))
    send_far[...] = total.astype(BF16).reshape(8, 8, 512)

    with scope("w_ready23"):
        pl.semaphore_wait(ready.at[2], 1)
        pl.semaphore_wait(ready.at[3], 1)
    rfar = {}

    def far_sums(*slots):
        for k in slots:
            rfar[k] = send(send_far.at[lax.rem(j + k, 8)], far_in.at[k], rfar_send.at[k], rfar_recv.at[k], along(4 * k))

    far_sums(4, 3, 5)
    await_far(1)
    near_forward(1)
    await_far(7)
    near_forward(7)
    await_far(2)
    afar[4] = far_pass(2, 4, 8)
    afar[3] = far_pass(2, 3, 4)
    near_forward(2)
    await_far(6)
    afar[5] = far_pass(6, 5, -4)
    far_sums(2, 6, 1, 7)
    near_forward(6)

    await_plane(1)
    plane[4] = pass_on(1, 4, 0, 1)
    plane[5] = pass_on(1, 5, 0, 3)
    pairs.append(to_pair(1, 1))

    await_plane(6)
    plane[7] = pass_on(6, 7, 1, 0, low)
    await_plane(8)
    plane[9] = pass_on(6, 9, 1, 0, high)
    pairs.append(to_pair(6, 6))

    await_far(3)
    near_forward(3)
    await_far(5)
    near_forward(5)

    await_plane(4)
    pairs.append(to_pair(4, 4))
    await_plane(5)
    pairs.append(to_pair(5, 5))
    await_far(4)
    near_forward(4)
    await_plane(7)
    pairs.append(to_pair(7, 7, low))
    await_plane(9)
    pairs.append(to_pair(7, 8, high))
    with scope("w_pairs"):
        for copy in pairs:
            copy.wait_recv()

    row, col = iota((256, 256), 0), iota((256, 256), 1)
    regroup = one_hot(col == ((row >> 1) & 15) * 16 + (row >> 5) * 2 + (row & 1))

    def weights(half, cls):
        x = dot(xall[half, cls].reshape(256, 128), regroup, ((0,), (0,))).astype(BF16)
        g = gall[:, cls, half].reshape(256, 896)
        return dot(x, g, ((1,), (0,)))

    acc[...] = weights(xh, r)

    for k in FAR:
        with scope(f"w_rfar{k}"):
            rfar[k].wait_recv()
    latent = send_far[j].astype(F32)
    for k in range(1, 8):
        latent = latent + far_in[k].astype(F32)
    for i in range(2):
        for q in range(4):
            natural[i : i + 1, 512 * q : 512 * q + 512] = latent[4 * i + q : 4 * i + q + 1, :]

    def norm_back(incoming, unit, inverse, gain):
        scaled = gain[...].reshape(1, -1) * incoming
        mean = jnp.mean(scaled * unit, axis=-1, keepdims=True)
        return inverse * (scaled - unit * mean)

    q_unit, q_inv, q_normed = norm(ql, qg)
    kv_unit, kv_inv, kv_normed = norm(kvl, kvg)
    dql[...] = norm_back(natural[:, 0:1536], q_unit, q_inv, qg)
    dkvl[...] = norm_back(natural[:, 1536:2048], kv_unit, kv_inv, kvg)

    outs = [
        pltpu.make_async_copy(src, dst, out_sem.at[n])
        for n, (src, dst) in enumerate([
            (dql, dql_hbm), (dkvl, dkvl_hbm), (acc.at[0:96, 0:384], dqup_hbm), (acc.at[96:128, 384:896], dkvup_hbm)])
    ]
    outs[0].start()
    outs[1].start()

    def near_copy(n, at):
        s, flip = NEAR[n]
        return pltpu.make_async_remote_copy(
            src_ref=at, dst_ref=at, send_sem=anear_send.at[n], recv_sem=anear_recv.at[n],
            device_id=along(steps[s], flip), device_id_type=MESH)

    places = []
    for n, (s, flip) in enumerate(NEAR):
        half = 1 - xh if flip else xh
        cls = lax.rem(z - steps[s] + 32, 4)
        places.append((half, cls))
        with scope(f"w_anear{n}"):
            near_copy(n, xall.at[half, cls]).wait_recv()
    with scope("c_weights"):
        total = acc[...]
        for half, cls in places:
            total = total + weights(half, cls)
        acc[...] = total
    outs[2].start()
    outs[3].start()

    with scope("w_sends"):
        for copy in mixes + list(plane.values()) + pairs + rnear + list(rfar.values()) + list(afar.values()):
            copy.wait_send()
        for n in range(7):
            near_copy(n, xall.at[xh, r]).wait_send()
    with scope("w_outs"):
        for out in outs:
            out.wait()


def write_kernel(a, b, w, v, dql, dkvl, dqup, dkvup, at, bt, wt, vt, sem_in, sem_out):
    stages = list(enumerate([(w, wt, dqup), (v, vt, dkvup), (a, at, dql), (b, bt, dkvl)]))
    ins = [pltpu.make_async_copy(src, mid, sem_in.at[n]) for n, (src, mid, dst) in stages]
    outs = [pltpu.make_async_copy(mid, dst, sem_out.at[n]) for n, (src, mid, dst) in stages]
    for copy in ins:
        copy.start()
    for copy, out in zip(ins, outs):
        copy.wait()
        out.start()
    for out in outs:
        out.wait()


def body(query_latent, key_value_latent, query_gain, key_value_gain, q_up, kv_up, grad_q, grad_kv):
    dma = pltpu.SemaphoreType.DMA
    vmem = pltpu.VMEM
    hbm = pl.BlockSpec(memory_space=pltpu.HBM)
    shapes = (
        jax.ShapeDtypeStruct((2, 1536), F32),
        jax.ShapeDtypeStruct((2, 512), F32),
        jax.ShapeDtypeStruct((96, 384), F32),
        jax.ShapeDtypeStruct((32, 512), F32),
    )
    results = pl.pallas_call(
        kernel,
        name="mla_up_backward",
        out_shape=shapes,
        in_specs=[hbm] * 8,
        out_specs=(hbm,) * 4,
        scratch_shapes=[
            vmem((2, 1536), BF16), vmem((2, 512), BF16), vmem((1536,), F32), vmem((512,), F32),
            vmem((1536, 384), BF16), vmem((512, 512), BF16), vmem((128, 896), BF16),
            vmem((16, 2, 128), F32),
            vmem((16, 2, 128), F32),
            vmem((32, 128), F32),
            vmem((16, 4, 2, 16, 896), BF16),
            vmem((2, 4, 8, 32, 128), BF16),
            vmem((4, 2, 4, 16, 512), BF16),
            vmem((7, 4, 16, 512), BF16),
            vmem((8, 8, 512), BF16),
            vmem((8, 8, 512), BF16),
            vmem((2, 2048), F32),
            vmem((128, 896), F32),
            dma((8,)), dma((16,)), dma((16,)), dma((10,)), dma((10,)), dma((9,)), dma((9,)),
            dma((7,)), dma((7,)), dma((8,)), dma((8,)), dma((8,)), dma((8,)), dma((7,)), dma((7,)),
            vmem((2, 1536), F32), vmem((2, 512), F32), dma((4,)),
            pltpu.SemaphoreType.REGULAR((4,)),
        ],
        compiler_params=pltpu.CompilerParams(
            collective_id=0, has_side_effects=True, vmem_limit_bytes=67043328),
    )(query_latent, key_value_latent, query_gain, key_value_gain, q_up, kv_up, grad_q, grad_kv)
    return pl.pallas_call(
        write_kernel,
        name="write_results",
        out_shape=shapes,
        in_specs=[hbm] * 4,
        out_specs=(hbm,) * 4,
        scratch_shapes=[vmem(shape.shape, F32) for shape in shapes] + [dma((4,)), dma((4,))],
        compiler_params=pltpu.CompilerParams(vmem_limit_bytes=67043328),
    )(*results)


def solution(mesh):
    group = ("dp", "tensor")
    placed = (
        P(group, None), P(group, None), P(), P(), P(None, "tensor"), P(None, "tensor"),
        P("dp", "tensor"), P("dp", "tensor"),
    )
    return jax.shard_map(
        body,
        mesh=mesh,
        in_specs=placed,
        out_specs=(P(group, None), P(group, None), P("dp", "tensor"), P("dp", "tensor")),
        check_vma=False,
    )
```

```python
import jax
import jax.numpy as jnp
from jax import lax
from jax.experimental import pallas as pl
from jax.experimental.pallas import tpu as pltpu
from jax.sharding import PartitionSpec as P

MESH = pl.DeviceIdType.MESH
F32 = jnp.float32
BF16 = jnp.bfloat16
EPS = 1e-06
scope = jax.named_scope

NEAR = [(1, 0), (2, 0), (3, 0), (0, 1), (1, 1), (2, 1), (3, 1)]
FAR = [1, 7, 2, 6, 3, 5, 4]
PLANE = [(0, 0), (1, 0), (0, 3), (0, 1), (1, 3), (1, 1), (0, 2), (1, 2)]


def iota(shape, dim):
    return lax.broadcasted_iota(jnp.int32, shape, dim)


def one_hot(mask):
    return jnp.where(mask, 1.0, 0.0).astype(BF16)


def dot(a, b, dims):
    return lax.dot_general(a, b, (dims, ((), ())), preferred_element_type=F32)


def kernel(
    ql_hbm, kvl_hbm, qg_hbm, kvg_hbm, qup_hbm, kvup_hbm, gq_hbm, gkv_hbm,
    dql, dkvl, dqup, dkvup,
    ql, kvl, qg, kvg, qup, kvup, grads,
    pack, mixed, piece, gall, xall, part, near_in, send_far, far_in, natural, acc,
    load_sem, mix_send, mix_recv, plane_send, plane_recv, pair_send, pair_recv,
    rnear_send, rnear_recv, rfar_send, rfar_recv, afar_send, afar_recv, anear_send, anear_recv,
    ready,
):
    dp, tensor = lax.axis_index("dp"), lax.axis_index("tensor")
    c = lax.rem(dp, 2)
    y = lax.rem(dp // 2, 4)
    xl = dp // 8
    z = lax.rem(tensor, 32)
    xh = tensor // 32
    r = lax.rem(z, 4)
    j = z // 4
    width = 4 * c - 2
    steps = [0, 1, -1, width]

    def along(dz, flip=0):
        half = 1 - xh if flip else xh
        return (dp, half * 32 + lax.rem(z + dz + 32, 32))

    def chip(dx, dy, other=0):
        px = 1 - xl if dx else xl
        core = 1 - c if other else c
        return (px * 4 + lax.rem(y + dy, 4)) * 2 + core

    barrier = pltpu.get_barrier_semaphore()
    peers = [along(4), along(-4)]
    peers += [along(dz, flip) for flip in (1, 0) for dz in (2, -2, 1, -1)]
    peers += [(lax.rem(dp + k, 16), tensor) for k in range(15, 0, -1)]
    peers += [along(0, 1)]
    for peer in peers[:10]:
        pl.semaphore_signal(barrier, inc=1, device_id=peer, device_id_type=MESH)

    loads = [
        pltpu.make_async_copy(src, dst, load_sem.at[min(n, 4) if n < 6 else n - 1])
        for n, (src, dst) in enumerate([
            (ql_hbm, ql), (kvl_hbm, kvl), (qg_hbm, qg), (kvg_hbm, kvg),
            (gq_hbm, grads.at[:, 0:384]), (gkv_hbm, grads.at[:, 384:896]),
            (qup_hbm, qup), (kvup_hbm, kvup),
        ])
    ]
    for load in loads:
        load.start()
    for peer in peers[10:]:
        pl.semaphore_signal(barrier, inc=1, device_id=peer, device_id_type=MESH)
    sent = []

    def send(src, dst, send_sem, recv_sem, device):
        copy = pltpu.make_async_remote_copy(
            src_ref=src, dst_ref=dst, send_sem=send_sem, recv_sem=recv_sem,
            device_id=device, device_id_type=MESH)
        copy.start()
        return copy

    def everything(at, sem):
        return pltpu.make_async_copy(at, at, sem)

    with scope("w_loadsmall"):
        for load in loads[:4]:
            load.wait()

    def norm(raw, gain):
        wide = raw[...].astype(F32)
        inverse = lax.rsqrt(jnp.mean(wide * wide, axis=-1, keepdims=True) + EPS)
        unit = wide * inverse
        return unit, inverse, gain[...].reshape(1, -1) * unit

    q_unit, q_inv, q_normed = norm(ql, qg)
    kv_unit, kv_inv, kv_normed = norm(kvl, kvg)
    for b in range(16):
        pack[b, :, 0:96] = q_normed[:, 96 * b : 96 * b + 96]
        pack[b, :, 96:128] = kv_normed[:, 32 * b : 32 * b + 32]

    with scope("w_loadgrads"):
        everything(grads, load_sem.at[4]).wait()
    row, col = iota((128, 128), 0), iota((128, 128), 1)
    token = ((row >> 4) & 1) * 64 + ((row >> 1) & 7) * 8 + (row >> 5) * 2 + (row & 1)
    order = one_hot(col == token)
    ordered = dot(order, grads[...], ((1,), (0,))).astype(BF16)
    gall[dp] = ordered.reshape(4, 2, 16, 896)
    mixed[dp] = pack[dp]

    with scope("w_loadup"):
        loads[6].wait()
        loads[7].wait()
    own = gall[dp].reshape(128, 896)
    for q in range(4):
        if q < 3:
            value = dot(own[:, 0:384], qup[512 * q : 512 * q + 512, :], ((1,), (1,)))
        else:
            value = dot(own[:, 384:896], kvup[...], ((1,), (1,)))
        part[:, :, q] = value.astype(BF16).reshape(4, 2, 16, 512)

    with scope("w_barrier"):
        pl.semaphore_wait(barrier, len(peers))
    pl.semaphore_signal(ready.at[0], inc=1, device_id=along(-4), device_id_type=MESH)
    pl.semaphore_signal(ready.at[1], inc=1, device_id=along(4), device_id_type=MESH)

    mixes = []
    for k in range(1, 16):
        to = lax.rem(dp + k, 16)
        mixes.append(send(pack.at[to], mixed.at[dp], mix_send.at[0], mix_recv.at[0], (to, tensor)))

    whole, low, high = pl.ds(0, 4), pl.ds(0, 2), pl.ds(2, 2)

    def pass_on(n, slot, dx, dy, rows=whole):
        at = gall.at[chip(*PLANE[n]), rows]
        return send(at, at, plane_send.at[0], plane_recv.at[slot - 1], (chip(dx, dy), tensor))

    def to_pair(n, slot, rows=whole):
        at = gall.at[chip(*PLANE[n]), rows]
        return send(at, at, pair_send.at[0], pair_recv.at[0], (chip(0, 0, 1), tensor))

    rnear = []
    for n, (s, flip) in enumerate(NEAR):
        device = along(steps[s], flip)
        half = 1 - xh if flip else xh
        cls = lax.rem(z + steps[s] + 32, 4)
        rnear.append(send(part.at[cls, half], near_in.at[n], rnear_send.at[0], rnear_recv.at[0], device))

    plane = {}
    plane[2] = pass_on(0, 2, 0, 1)
    plane[3] = pass_on(0, 3, 0, 3)
    plane[1] = pass_on(0, 1, 1, 0)
    pairs = [to_pair(0, 0)]

    with scope("w_ready01"):
        pl.semaphore_wait(ready.at[0], 1)
        pl.semaphore_wait(ready.at[1], 1)
    pl.semaphore_signal(ready.at[2], inc=1, device_id=along(-8), device_id_type=MESH)
    pl.semaphore_signal(ready.at[3], inc=1, device_id=along(8), device_id_type=MESH)

    with scope("w_mixes"):
        everything(mixed.at[pl.ds(0, 15)], mix_recv.at[0]).wait()
    for b in range(16):
        piece[2 * b : 2 * b + 2, :] = mixed[b]
    xall[xh * 4 + r, j] = piece[...].astype(BF16)

    def far_pass(k, slot, dz):
        at = xall.at[xh * 4 + r, lax.rem(j + 8 - k, 8)]
        return send(at, at, afar_send.at[0], afar_recv.at[slot - 1], along(dz))

    def near_forward(k):
        at = xall.at[xh * 4 + r, lax.rem(j + 8 - k, 8)]
        for n, (s, flip) in enumerate(NEAR):
            send(at, at, anear_send.at[0], anear_recv.at[0], along(steps[s], flip))

    afar = {}
    afar[2] = far_pass(0, 2, 8)
    afar[6] = far_pass(0, 6, -8)
    afar[1] = far_pass(0, 1, 4)
    afar[7] = far_pass(0, 7, -4)
    near_forward(0)

    def await_plane(*slots):
        for slot in slots:
            with scope(f"w_plane{slot}"):
                plane[slot].wait_recv()

    def await_far(*slots):
        for slot in slots:
            with scope(f"w_afar{slot}"):
                afar[slot].wait_recv()

    await_plane(2)
    plane[6] = pass_on(2, 6, 0, 1, low)
    pairs.append(to_pair(2, 2))
    await_plane(3)
    plane[8] = pass_on(3, 8, 0, 3, high)
    pairs.append(to_pair(3, 3))
    with scope("w_rnear"):
        everything(near_in, rnear_recv.at[0]).wait()
    total = part[r, xh].astype(F32)
    for n in range(7):
        total = total + near_in[n].astype(F32)
    row, col = iota((64, 64), 0), iota((64, 64), 1)
    spread = one_hot(col == (row & 3) * 16 + (row >> 3) * 2 + ((row >> 2) & 1))
    total = dot(spread, total.astype(BF16).reshape(64, 512), ((1,), (0,)))
    send_far[...] = total.astype(BF16).reshape(8, 8, 512)

    with scope("w_ready23"):
        pl.semaphore_wait(ready.at[2], 1)
        pl.semaphore_wait(ready.at[3], 1)
    rfar = {}

    def far_sums(*slots):
        for k in slots:
            rfar[k] = send(send_far.at[lax.rem(j + k, 8)], far_in.at[k], rfar_send.at[0], rfar_recv.at[0], along(4 * k))

    far_sums(4)
    await_far(1)
    near_forward(1)
    await_far(7)
    near_forward(7)
    await_far(2)
    await_far(6)
    afar[4] = far_pass(2 + 4 * c, 4, 8 - 16 * c)
    afar[3] = far_pass(2, 3, 4)
    afar[5] = far_pass(6, 5, -4)
    far_sums(3, 5, 2, 6, 1, 7)
    near_forward(2)
    near_forward(6)

    await_plane(1)
    plane[4] = pass_on(1, 4, 0, 1)
    plane[5] = pass_on(1, 5, 0, 3)
    pairs.append(to_pair(1, 1))

    await_plane(6)
    plane[7] = pass_on(6, 7, 1, 0, low)
    await_plane(8)
    plane[9] = pass_on(6, 9, 1, 0, high)
    pairs.append(to_pair(6, 6))

    await_far(3)
    near_forward(3)
    await_far(5)
    near_forward(5)

    await_plane(4)
    pairs.append(to_pair(4, 4))
    await_plane(5)
    pairs.append(to_pair(5, 5))
    await_far(4)
    near_forward(4)
    await_plane(7)
    pairs.append(to_pair(7, 7, low))
    await_plane(9)
    pairs.append(to_pair(7, 8, high))
    with scope("w_pairs"):
        everything(gall.at[pl.ds(0, 8)], pair_recv.at[0]).wait()

    row, col = iota((256, 256), 0), iota((256, 256), 1)
    regroup = one_hot(col == ((row >> 1) & 15) * 16 + (row >> 5) * 2 + (row & 1))

    def weights(half, cls):
        x = dot(xall[half * 4 + cls].reshape(256, 128), regroup, ((0,), (0,))).astype(BF16)
        g = gall[:, cls, half].reshape(256, 896)
        return dot(x, g, ((1,), (0,)))

    acc[...] = weights(xh, r)

    with scope("w_rfar"):
        everything(far_in.at[pl.ds(1, 7)], rfar_recv.at[0]).wait()
    latent = send_far[j].astype(F32)
    for k in range(1, 8):
        latent = latent + far_in[k].astype(F32)
    for i in range(2):
        for q in range(4):
            natural[i : i + 1, 512 * q : 512 * q + 512] = latent[4 * i + q : 4 * i + q + 1, :]

    def norm_back(incoming, unit, inverse, gain):
        scaled = gain[...].reshape(1, -1) * incoming
        mean = jnp.mean(scaled * unit, axis=-1, keepdims=True)
        return inverse * (scaled - unit * mean)

    q_unit, q_inv, q_normed = norm(ql, qg)
    kv_unit, kv_inv, kv_normed = norm(kvl, kvg)
    dql[...] = norm_back(natural[:, 0:1536], q_unit, q_inv, qg)
    dkvl[...] = norm_back(natural[:, 1536:2048], kv_unit, kv_inv, kvg)

    places = []
    for n, (s, flip) in enumerate(NEAR):
        half = 1 - xh if flip else xh
        cls = lax.rem(z - steps[s] + 32, 4)
        places.append((half, cls))
    with scope("w_anear"):
        everything(xall.at[pl.ds(0, 7)], anear_recv.at[0]).wait()
    with scope("c_weights"):
        total = acc[...]
        for half, cls in places:
            total = total + weights(half, cls)
        dqup[...] = total[0:96, 0:384]
        dkvup[...] = total[96:128, 384:896]

    with scope("w_sends"):
        everything(mixed.at[pl.ds(0, 15)], mix_send.at[0]).wait()
        everything(gall.at[pl.ds(0, 7)], plane_send.at[0]).wait()
        everything(gall.at[pl.ds(0, 8)], pair_send.at[0]).wait()
        everything(near_in, rnear_send.at[0]).wait()
        everything(far_in.at[pl.ds(1, 7)], rfar_send.at[0]).wait()
        everything(xall.at[0, pl.ds(0, 7)], afar_send.at[0]).wait()
        everything(xall.at[pl.ds(0, 7)], anear_send.at[0]).wait()


def write_kernel(a, b, w, v, dql, dkvl, dqup, dkvup, sem):
    copies = [
        pltpu.make_async_copy(src, dst, sem.at[n])
        for n, (src, dst) in enumerate([(w, dqup), (v, dkvup), (a, dql), (b, dkvl)])
    ]
    for copy in copies:
        copy.start()
    for copy in copies:
        copy.wait()


def body(query_latent, key_value_latent, query_gain, key_value_gain, q_up, kv_up, grad_q, grad_kv):
    dma = pltpu.SemaphoreType.DMA
    vmem = pltpu.VMEM
    hbm = pl.BlockSpec(memory_space=pltpu.HBM)
    shapes = (
        jax.ShapeDtypeStruct((2, 1536), F32),
        jax.ShapeDtypeStruct((2, 512), F32),
        jax.ShapeDtypeStruct((96, 384), F32),
        jax.ShapeDtypeStruct((32, 512), F32),
    )
    results = pl.pallas_call(
        kernel,
        name="mla_up_backward",
        out_shape=tuple(vmem(shape.shape, F32) for shape in shapes),
        in_specs=[hbm] * 8,
        out_specs=(pl.BlockSpec(memory_space=pltpu.VMEM),) * 4,
        scratch_shapes=[
            vmem((2, 1536), BF16), vmem((2, 512), BF16), vmem((1536,), F32), vmem((512,), F32),
            vmem((1536, 384), BF16), vmem((512, 512), BF16), vmem((128, 896), BF16),
            vmem((16, 2, 128), F32),
            vmem((16, 2, 128), F32),
            vmem((32, 128), F32),
            vmem((16, 4, 2, 16, 896), BF16),
            vmem((8, 8, 32, 128), BF16),
            vmem((4, 2, 4, 16, 512), BF16),
            vmem((7, 4, 16, 512), BF16),
            vmem((8, 8, 512), BF16),
            vmem((8, 8, 512), BF16),
            vmem((2, 2048), F32),
            vmem((128, 896), F32),
            dma((7,)), dma((1,)), dma((1,)), dma((1,)), dma((9,)), dma((1,)), dma((1,)),
            dma((1,)), dma((1,)), dma((1,)), dma((1,)), dma((1,)), dma((7,)), dma((1,)), dma((1,)),
            pltpu.SemaphoreType.REGULAR((4,)),
        ],
        compiler_params=pltpu.CompilerParams(
            collective_id=0, has_side_effects=True, vmem_limit_bytes=60 * 1000 * 1000),
    )(query_latent, key_value_latent, query_gain, key_value_gain, q_up, kv_up, grad_q, grad_kv)
    return pl.pallas_call(
        write_kernel,
        name="write_results",
        out_shape=shapes,
        in_specs=[pl.BlockSpec(memory_space=pltpu.VMEM)] * 4,
        out_specs=(hbm,) * 4,
        scratch_shapes=[dma((4,))],
        compiler_params=pltpu.CompilerParams(vmem_limit_bytes=1024 * 1024),
    )(*results)


def solution(mesh):
    group = ("dp", "tensor")
    placed = (
        P(group, None), P(group, None), P(), P(), P(None, "tensor"), P(None, "tensor"),
        P("dp", "tensor"), P("dp", "tensor"),
    )
    return jax.shard_map(
        body,
        mesh=mesh,
        in_specs=placed,
        out_specs=(P(group, None), P(group, None), P("dp", "tensor"), P("dp", "tensor")),
        check_vma=False,
    )
```

```python
import jax
import jax.numpy as jnp
from jax import lax
from jax.experimental import pallas as pl
from jax.experimental.pallas import tpu as pltpu
from jax.sharding import PartitionSpec as P

MESH = pl.DeviceIdType.MESH
F32 = jnp.float32
BF16 = jnp.bfloat16
EPS = 1e-06
scope = jax.named_scope

NEAR = [(1, 0), (2, 0), (3, 0), (0, 1), (1, 1), (2, 1), (3, 1)]
FAR = [1, 7, 2, 6, 3, 5, 4]
PLANE = [(0, 0), (1, 0), (0, 3), (0, 1), (1, 3), (1, 1), (0, 2), (1, 2)]


def iota(shape, dim):
    return lax.broadcasted_iota(jnp.int32, shape, dim)


def one_hot(mask):
    return jnp.where(mask, 1.0, 0.0).astype(BF16)


def dot(a, b, dims):
    return lax.dot_general(a, b, (dims, ((), ())), preferred_element_type=F32)


def kernel(
    ql_hbm, kvl_hbm, qg_hbm, kvg_hbm, qup_hbm, kvup_hbm, gq_hbm, gkv_hbm,
    dql, dkvl, dqup, dkvup,
    ql, kvl, qg, kvg, qup, kvup, grads,
    pack, mixed, piece, gall, xall, xlate, glate, part, near_in, send_far, far_in, natural, acc,
    load_sem, mix_send, mix_recv, plane_send, plane_recv, pair_send, pair_recv,
    rnear_send, rnear_recv, rfar_send, rfar_recv, afar_send, afar_recv, anear_send, anear_recv,
    ready,
):
    dp, tensor = lax.axis_index("dp"), lax.axis_index("tensor")
    c = lax.rem(dp, 2)
    y = lax.rem(dp // 2, 4)
    xl = dp // 8
    z = lax.rem(tensor, 32)
    xh = tensor // 32
    r = lax.rem(z, 4)
    j = z // 4
    width = 4 * c - 2
    steps = [0, 1, -1, width]

    def along(dz, flip=0):
        half = 1 - xh if flip else xh
        return (dp, half * 32 + lax.rem(z + dz + 32, 32))

    def chip(dx, dy, other=0):
        px = 1 - xl if dx else xl
        core = 1 - c if other else c
        return (px * 4 + lax.rem(y + dy, 4)) * 2 + core

    barrier = pltpu.get_barrier_semaphore()
    peers = [along(4), along(-4)]
    peers += [along(dz, flip) for flip in (1, 0) for dz in (2, -2, 1, -1)]
    peers += [(lax.rem(dp + k, 16), tensor) for k in range(15, 0, -1)]
    peers += [along(0, 1)]
    for peer in peers[:10]:
        pl.semaphore_signal(barrier, inc=1, device_id=peer, device_id_type=MESH)

    loads = [
        pltpu.make_async_copy(src, dst, load_sem.at[min(n, 4) if n < 6 else n - 1])
        for n, (src, dst) in enumerate([
            (ql_hbm, ql), (kvl_hbm, kvl), (qg_hbm, qg), (kvg_hbm, kvg),
            (gq_hbm, grads.at[:, 0:384]), (gkv_hbm, grads.at[:, 384:896]),
            (qup_hbm, qup), (kvup_hbm, kvup),
        ])
    ]
    for load in loads:
        load.start()
    for peer in peers[10:]:
        pl.semaphore_signal(barrier, inc=1, device_id=peer, device_id_type=MESH)
    sent = []

    def send(src, dst, send_sem, recv_sem, device):
        copy = pltpu.make_async_remote_copy(
            src_ref=src, dst_ref=dst, send_sem=send_sem, recv_sem=recv_sem,
            device_id=device, device_id_type=MESH)
        copy.start()
        return copy

    def everything(at, sem):
        return pltpu.make_async_copy(at, at, sem)

    with scope("w_loadsmall"):
        for load in loads[:4]:
            load.wait()

    def norm(raw, gain):
        wide = raw[...].astype(F32)
        inverse = lax.rsqrt(jnp.mean(wide * wide, axis=-1, keepdims=True) + EPS)
        unit = wide * inverse
        return unit, inverse, gain[...].reshape(1, -1) * unit

    q_unit, q_inv, q_normed = norm(ql, qg)
    kv_unit, kv_inv, kv_normed = norm(kvl, kvg)
    for b in range(16):
        pack[b, :, 0:96] = q_normed[:, 96 * b : 96 * b + 96]
        pack[b, :, 96:128] = kv_normed[:, 32 * b : 32 * b + 32]

    with scope("w_loadgrads"):
        everything(grads, load_sem.at[4]).wait()
    row, col = iota((128, 128), 0), iota((128, 128), 1)
    token = ((row >> 4) & 1) * 64 + ((row >> 1) & 7) * 8 + (row >> 5) * 2 + (row & 1)
    order = one_hot(col == token)
    ordered = dot(order, grads[...], ((1,), (0,))).astype(BF16)
    gall[dp] = ordered.reshape(4, 2, 16, 896)
    mixed[dp] = pack[dp]

    with scope("w_loadup"):
        loads[6].wait()
        loads[7].wait()
    own = gall[dp].reshape(128, 896)
    for q in range(4):
        if q < 3:
            value = dot(own[:, 0:384], qup[512 * q : 512 * q + 512, :], ((1,), (1,)))
        else:
            value = dot(own[:, 384:896], kvup[...], ((1,), (1,)))
        part[:, :, q] = value.astype(BF16).reshape(4, 2, 16, 512)

    classes = []
    for s, flip in [(0, 0)] + NEAR:
        at = lax.rem(z - steps[s] + 32, 32)
        late = [lax.rem(at // 4 + 8 - k, 8) for k in (3, 4, 5)]
        classes.append((1 - xh if flip else xh, lax.rem(at, 4), late))
    for half, cls, late in classes:
        for place in late:
            xall[half * 4 + cls, place] = jnp.zeros((32, 128), BF16)

    with scope("w_barrier"):
        pl.semaphore_wait(barrier, len(peers))
    pl.semaphore_signal(ready.at[0], inc=1, device_id=along(-4), device_id_type=MESH)
    pl.semaphore_signal(ready.at[1], inc=1, device_id=along(4), device_id_type=MESH)

    mixes = []
    for k in range(1, 16):
        to = lax.rem(dp + k, 16)
        mixes.append(send(pack.at[to], mixed.at[dp], mix_send.at[0], mix_recv.at[0], (to, tensor)))

    whole, low, high = pl.ds(0, 4), pl.ds(0, 2), pl.ds(2, 2)

    def pass_on(n, slot, dx, dy, rows=whole):
        at = gall.at[chip(*PLANE[n]), rows]
        return send(at, at, plane_send.at[0], plane_recv.at[slot - 1], (chip(dx, dy), tensor))

    def to_pair(n, slot, rows=whole):
        at = gall.at[chip(*PLANE[n]), rows]
        return send(at, at, pair_send.at[0], pair_recv.at[0], (chip(0, 0, 1), tensor))

    rnear = []
    for n, (s, flip) in enumerate(NEAR):
        device = along(steps[s], flip)
        half = 1 - xh if flip else xh
        cls = lax.rem(z + steps[s] + 32, 4)
        rnear.append(send(part.at[cls, half], near_in.at[n], rnear_send.at[0], rnear_recv.at[0], device))

    plane = {}
    plane[2] = pass_on(0, 2, 0, 1)
    plane[3] = pass_on(0, 3, 0, 3)
    plane[1] = pass_on(0, 1, 1, 0)
    pairs = [to_pair(0, 0)]

    with scope("w_ready01"):
        pl.semaphore_wait(ready.at[0], 1)
        pl.semaphore_wait(ready.at[1], 1)
    pl.semaphore_signal(ready.at[2], inc=1, device_id=along(-8), device_id_type=MESH)
    pl.semaphore_signal(ready.at[3], inc=1, device_id=along(8), device_id_type=MESH)

    with scope("w_mixes"):
        everything(mixed.at[pl.ds(0, 15)], mix_recv.at[0]).wait()
    for b in range(16):
        piece[2 * b : 2 * b + 2, :] = mixed[b]
    xall[xh * 4 + r, j] = piece[...].astype(BF16)

    mine = xh * 4 + r

    def far_pass(k, slot, dz):
        at = xall.at[mine, lax.rem(j + 8 - k, 8)]
        to = xlate.at[slot - 3, mine] if slot in (3, 4, 5) else at
        return send(at, to, afar_send.at[0], afar_recv.at[slot - 1], along(dz))

    def near_forward(k):
        late = 1 if k in (3, 4, 5) else 0
        at = xlate.at[k - 3, mine] if late else xall.at[mine, lax.rem(j + 8 - k, 8)]
        for s, flip in NEAR:
            send(at, at, anear_send.at[late], anear_recv.at[late], along(steps[s], flip))

    afar = {}
    afar[2] = far_pass(0, 2, 8)
    afar[6] = far_pass(0, 6, -8)
    afar[1] = far_pass(0, 1, 4)
    afar[7] = far_pass(0, 7, -4)
    near_forward(0)

    def await_plane(*slots):
        for slot in slots:
            with scope(f"w_plane{slot}"):
                plane[slot].wait_recv()

    def await_far(*slots):
        for slot in slots:
            with scope(f"w_afar{slot}"):
                afar[slot].wait_recv()

    await_plane(2)
    plane[6] = pass_on(2, 6, 0, 1, low)
    pairs.append(to_pair(2, 2))
    await_plane(3)
    plane[8] = pass_on(3, 8, 0, 3, high)
    pairs.append(to_pair(3, 3))
    with scope("w_rnear"):
        everything(near_in, rnear_recv.at[0]).wait()
    total = part[r, xh].astype(F32)
    for n in range(7):
        total = total + near_in[n].astype(F32)
    row, col = iota((64, 64), 0), iota((64, 64), 1)
    spread = one_hot(col == (row & 3) * 16 + (row >> 3) * 2 + ((row >> 2) & 1))
    total = dot(spread, total.astype(BF16).reshape(64, 512), ((1,), (0,)))
    send_far[...] = total.astype(BF16).reshape(8, 8, 512)

    with scope("w_ready23"):
        pl.semaphore_wait(ready.at[2], 1)
        pl.semaphore_wait(ready.at[3], 1)
    rfar = {}

    def far_sums(*slots):
        for k in slots:
            rfar[k] = send(send_far.at[lax.rem(j + k, 8)], far_in.at[k], rfar_send.at[0], rfar_recv.at[0], along(4 * k))

    far_sums(4)
    await_far(1)
    near_forward(1)
    await_far(7)
    near_forward(7)
    await_far(2)
    await_far(6)
    afar[4] = far_pass(2 + 4 * c, 4, 8 - 16 * c)
    afar[3] = far_pass(2, 3, 4)
    afar[5] = far_pass(6, 5, -4)
    far_sums(3, 5, 2, 6, 1, 7)
    near_forward(2)
    near_forward(6)

    await_plane(1)
    plane[4] = pass_on(1, 4, 0, 1)
    plane[5] = pass_on(1, 5, 0, 3)
    pairs.append(to_pair(1, 1))

    await_plane(6)
    plane[7] = pass_on(6, 7, 1, 0, low)
    await_plane(8)
    plane[9] = pass_on(6, 9, 1, 0, high)
    pairs.append(to_pair(6, 6))

    await_far(3)
    near_forward(3)
    await_far(5)
    near_forward(5)
    await_far(4)
    near_forward(4)

    await_plane(4)
    pairs.append(to_pair(4, 4))
    await_plane(5)
    pairs.append(to_pair(5, 5))
    await_plane(7)
    pairs.append(to_pair(7, 7, low))
    await_plane(9)
    pairs.append(to_pair(7, 8, high))
    with scope("w_pairs"):
        everything(gall.at[pl.ds(0, 8)], pair_recv.at[0]).wait()

    row, col = iota((256, 256), 0), iota((256, 256), 1)
    regroup = one_hot(col == ((row >> 1) & 15) * 16 + (row >> 5) * 2 + (row & 1))

    def weights(half, cls):
        x = dot(xall[half * 4 + cls].reshape(256, 128), regroup, ((0,), (0,))).astype(BF16)
        g = gall[:, cls, half].reshape(256, 896)
        return dot(x, g, ((1,), (0,)))

    acc[...] = weights(xh, r)
    row, col = iota((32, 256), 0), iota((32, 256), 1)
    for half, cls, late in classes:
        for n, place in enumerate(late):
            pick = one_hot(col == (row >> 1) * 16 + 2 * place + (row & 1))
            glate[n, half * 4 + cls] = dot(pick, gall[:, cls, half].reshape(256, 896), ((1,), (0,))).astype(BF16)

    with scope("w_anear"):
        everything(xall.at[pl.ds(0, 7), pl.ds(0, 5)], anear_recv.at[0]).wait()
    with scope("c_weights"):
        total = acc[...]
        for half, cls, late in classes[1:]:
            total = total + weights(half, cls)
        acc[...] = total

    with scope("w_rfar"):
        everything(far_in.at[pl.ds(1, 7)], rfar_recv.at[0]).wait()
    latent = send_far[j].astype(F32)
    for k in range(1, 8):
        latent = latent + far_in[k].astype(F32)
    for i in range(2):
        for q in range(4):
            natural[i : i + 1, 512 * q : 512 * q + 512] = latent[4 * i + q : 4 * i + q + 1, :]

    def norm_back(incoming, unit, inverse, gain):
        scaled = gain[...].reshape(1, -1) * incoming
        mean = jnp.mean(scaled * unit, axis=-1, keepdims=True)
        return inverse * (scaled - unit * mean)

    q_unit, q_inv, q_normed = norm(ql, qg)
    kv_unit, kv_inv, kv_normed = norm(kvl, kvg)
    dql[...] = norm_back(natural[:, 0:1536], q_unit, q_inv, qg)
    dkvl[...] = norm_back(natural[:, 1536:2048], kv_unit, kv_inv, kvg)

    with scope("w_late"):
        everything(xlate.at[:, pl.ds(0, 7)], anear_recv.at[1]).wait()
    with scope("c_late"):
        total = acc[...]
        for n in range(3):
            total = total + dot(xlate[n].reshape(256, 128), glate[n].reshape(256, 896), ((0,), (0,)))
        dqup[...] = total[0:96, 0:384]
        dkvup[...] = total[96:128, 384:896]

    with scope("w_sends"):
        everything(mixed.at[pl.ds(0, 15)], mix_send.at[0]).wait()
        everything(gall.at[pl.ds(0, 7)], plane_send.at[0]).wait()
        everything(gall.at[pl.ds(0, 8)], pair_send.at[0]).wait()
        everything(near_in, rnear_send.at[0]).wait()
        everything(far_in.at[pl.ds(1, 7)], rfar_send.at[0]).wait()
        everything(xall.at[0, pl.ds(0, 7)], afar_send.at[0]).wait()
        everything(xall.at[pl.ds(0, 7), pl.ds(0, 5)], anear_send.at[0]).wait()
        everything(xlate.at[:, pl.ds(0, 7)], anear_send.at[1]).wait()


def write_kernel(a, b, w, v, dql, dkvl, dqup, dkvup, sem):
    copies = [
        pltpu.make_async_copy(src, dst, sem.at[n])
        for n, (src, dst) in enumerate([(w, dqup), (v, dkvup), (a, dql), (b, dkvl)])
    ]
    for copy in copies:
        copy.start()
    for copy in copies:
        copy.wait()


def body(query_latent, key_value_latent, query_gain, key_value_gain, q_up, kv_up, grad_q, grad_kv):
    dma = pltpu.SemaphoreType.DMA
    vmem = pltpu.VMEM
    hbm = pl.BlockSpec(memory_space=pltpu.HBM)
    shapes = (
        jax.ShapeDtypeStruct((2, 1536), F32),
        jax.ShapeDtypeStruct((2, 512), F32),
        jax.ShapeDtypeStruct((96, 384), F32),
        jax.ShapeDtypeStruct((32, 512), F32),
    )
    results = pl.pallas_call(
        kernel,
        name="mla_up_backward",
        out_shape=tuple(vmem(shape.shape, F32) for shape in shapes),
        in_specs=[hbm] * 8,
        out_specs=(pl.BlockSpec(memory_space=pltpu.VMEM),) * 4,
        scratch_shapes=[
            vmem((2, 1536), BF16), vmem((2, 512), BF16), vmem((1536,), F32), vmem((512,), F32),
            vmem((1536, 384), BF16), vmem((512, 512), BF16), vmem((128, 896), BF16),
            vmem((16, 2, 128), F32),
            vmem((16, 2, 128), F32),
            vmem((32, 128), F32),
            vmem((16, 4, 2, 16, 896), BF16),
            vmem((8, 8, 32, 128), BF16),
            vmem((3, 8, 32, 128), BF16),
            vmem((3, 8, 32, 896), BF16),
            vmem((4, 2, 4, 16, 512), BF16),
            vmem((7, 4, 16, 512), BF16),
            vmem((8, 8, 512), BF16),
            vmem((8, 8, 512), BF16),
            vmem((2, 2048), F32),
            vmem((128, 896), F32),
            dma((7,)), dma((1,)), dma((1,)), dma((1,)), dma((9,)), dma((1,)), dma((1,)),
            dma((1,)), dma((1,)), dma((1,)), dma((1,)), dma((1,)), dma((7,)), dma((2,)), dma((2,)),
            pltpu.SemaphoreType.REGULAR((4,)),
        ],
        compiler_params=pltpu.CompilerParams(
            collective_id=0, has_side_effects=True, vmem_limit_bytes=60 * 1000 * 1000),
    )(query_latent, key_value_latent, query_gain, key_value_gain, q_up, kv_up, grad_q, grad_kv)
    return pl.pallas_call(
        write_kernel,
        name="write_results",
        out_shape=shapes,
        in_specs=[pl.BlockSpec(memory_space=pltpu.VMEM)] * 4,
        out_specs=(hbm,) * 4,
        scratch_shapes=[dma((4,))],
        compiler_params=pltpu.CompilerParams(vmem_limit_bytes=1024 * 1024),
    )(*results)


def solution(mesh):
    group = ("dp", "tensor")
    placed = (
        P(group, None), P(group, None), P(), P(), P(None, "tensor"), P(None, "tensor"),
        P("dp", "tensor"), P("dp", "tensor"),
    )
    return jax.shard_map(
        body,
        mesh=mesh,
        in_specs=placed,
        out_specs=(P(group, None), P(group, None), P("dp", "tensor"), P("dp", "tensor")),
        check_vma=False,
    )
```

```python
import jax
import jax.numpy as jnp
from jax import lax
from jax.experimental import pallas as pl
from jax.experimental.pallas import tpu as pltpu
from jax.sharding import PartitionSpec as P

MESH = pl.DeviceIdType.MESH
F32 = jnp.float32
BF16 = jnp.bfloat16
EPS = 1e-06
scope = jax.named_scope

NEAR = [(1, 0), (2, 0), (3, 0), (0, 1), (1, 1), (2, 1), (3, 1)]
FAR = [1, 7, 2, 6, 3, 5, 4]
PLANE = [(0, 0), (1, 0), (0, 3), (0, 1), (1, 3), (1, 1), (0, 2), (1, 2)]


def iota(shape, dim):
    return lax.broadcasted_iota(jnp.int32, shape, dim)


def one_hot(mask):
    return jnp.where(mask, 1.0, 0.0).astype(BF16)


def dot(a, b, dims):
    return lax.dot_general(a, b, (dims, ((), ())), preferred_element_type=F32)


def kernel(
    ql_hbm, kvl_hbm, qg_hbm, kvg_hbm, qup_hbm, kvup_hbm, gq_hbm, gkv_hbm,
    dql, dkvl, dqup, dkvup,
    ql, kvl, qg, kvg, qup, kvup, grads,
    pack, mixed, piece, gall, xall, xlate, glate, part, near_in, send_far, far_in, natural, acc,
    load_sem, mix_send, mix_recv, plane_send, plane_recv, pair_send, pair_recv,
    rnear_send, rnear_recv, rfar_send, rfar_recv, afar_send, afar_recv, anear_send, anear_recv,
    ready,
):
    dp, tensor = lax.axis_index("dp"), lax.axis_index("tensor")
    c = lax.rem(dp, 2)
    y = lax.rem(dp // 2, 4)
    xl = dp // 8
    z = lax.rem(tensor, 32)
    xh = tensor // 32
    r = lax.rem(z, 4)
    j = z // 4
    width = 4 * c - 2
    steps = [0, 1, -1, width]

    def along(dz, flip=0):
        half = 1 - xh if flip else xh
        return (dp, half * 32 + lax.rem(z + dz + 32, 32))

    def chip(dx, dy, other=0):
        px = 1 - xl if dx else xl
        core = 1 - c if other else c
        return (px * 4 + lax.rem(y + dy, 4)) * 2 + core

    barrier = pltpu.get_barrier_semaphore()
    peers = [along(4), along(-4)]
    peers += [along(dz, flip) for flip in (1, 0) for dz in (2, -2, 1, -1)]
    peers += [(lax.rem(dp + k, 16), tensor) for k in range(15, 0, -1)]
    peers += [along(0, 1)]
    for peer in peers[:10]:
        pl.semaphore_signal(barrier, inc=1, device_id=peer, device_id_type=MESH)

    loads = [
        pltpu.make_async_copy(src, dst, load_sem.at[min(n, 4) if n < 6 else n - 1])
        for n, (src, dst) in enumerate([
            (ql_hbm, ql), (kvl_hbm, kvl), (qg_hbm, qg), (kvg_hbm, kvg),
            (gq_hbm, grads.at[:, 0:384]), (gkv_hbm, grads.at[:, 384:896]),
            (qup_hbm, qup), (kvup_hbm, kvup),
        ])
    ]
    for load in loads:
        load.start()
    for peer in peers[10:]:
        pl.semaphore_signal(barrier, inc=1, device_id=peer, device_id_type=MESH)
    sent = []

    def send(src, dst, send_sem, recv_sem, device):
        copy = pltpu.make_async_remote_copy(
            src_ref=src, dst_ref=dst, send_sem=send_sem, recv_sem=recv_sem,
            device_id=device, device_id_type=MESH)
        copy.start()
        return copy

    def everything(at, sem):
        return pltpu.make_async_copy(at, at, sem)

    with scope("w_loadsmall"):
        for load in loads[:4]:
            load.wait()

    def norm(raw, gain):
        wide = raw[...].astype(F32)
        inverse = lax.rsqrt(jnp.mean(wide * wide, axis=-1, keepdims=True) + EPS)
        unit = wide * inverse
        return unit, inverse, gain[...].reshape(1, -1) * unit

    q_unit, q_inv, q_normed = norm(ql, qg)
    kv_unit, kv_inv, kv_normed = norm(kvl, kvg)
    for b in range(16):
        pack[b, :, 0:96] = q_normed[:, 96 * b : 96 * b + 96]
        pack[b, :, 96:128] = kv_normed[:, 32 * b : 32 * b + 32]

    with scope("w_loadgrads"):
        everything(grads, load_sem.at[4]).wait()
    row, col = iota((128, 128), 0), iota((128, 128), 1)
    token = ((row >> 4) & 1) * 64 + ((row >> 1) & 7) * 8 + (row >> 5) * 2 + (row & 1)
    order = one_hot(col == token)
    ordered = dot(order, grads[...], ((1,), (0,))).astype(BF16)
    gall[dp] = ordered.reshape(4, 2, 16, 896)
    mixed[dp] = pack[dp]

    with scope("w_loadup"):
        loads[6].wait()
        loads[7].wait()
    own = gall[dp].reshape(128, 896)
    for q in range(4):
        if q < 3:
            value = dot(own[:, 0:384], qup[512 * q : 512 * q + 512, :], ((1,), (1,)))
        else:
            value = dot(own[:, 384:896], kvup[...], ((1,), (1,)))
        part[:, :, q] = value.astype(BF16).reshape(4, 2, 16, 512)

    classes = []
    for s, flip in [(0, 0)] + NEAR:
        at = lax.rem(z - steps[s] + 32, 32)
        late = [lax.rem(at // 4 + 8 - k, 8) for k in (3, 4, 5)]
        classes.append((1 - xh if flip else xh, lax.rem(at, 4), late))
    for half, cls, late in classes:
        for place in late:
            xall[half * 4 + cls, place] = jnp.zeros((32, 128), BF16)

    with scope("w_barrier"):
        pl.semaphore_wait(barrier, len(peers))
    pl.semaphore_signal(ready.at[0], inc=1, device_id=along(-4), device_id_type=MESH)
    pl.semaphore_signal(ready.at[1], inc=1, device_id=along(4), device_id_type=MESH)

    mixes = []
    for k in range(1, 16):
        to = lax.rem(dp + k, 16)
        mixes.append(send(pack.at[to], mixed.at[dp], mix_send.at[0], mix_recv.at[0], (to, tensor)))

    whole, low, high = pl.ds(0, 4), pl.ds(0, 2), pl.ds(2, 2)

    def pass_on(n, slot, dx, dy, rows=whole):
        at = gall.at[chip(*PLANE[n]), rows]
        return send(at, at, plane_send.at[0], plane_recv.at[slot - 1], (chip(dx, dy), tensor))

    def to_pair(n, slot, rows=whole):
        at = gall.at[chip(*PLANE[n]), rows]
        return send(at, at, pair_send.at[0], pair_recv.at[0], (chip(0, 0, 1), tensor))

    rnear = []
    for n, (s, flip) in enumerate(NEAR):
        device = along(steps[s], flip)
        half = 1 - xh if flip else xh
        cls = lax.rem(z + steps[s] + 32, 4)
        rnear.append(send(part.at[cls, half], near_in.at[n], rnear_send.at[0], rnear_recv.at[0], device))

    plane = {}
    plane[2] = pass_on(0, 2, 0, 1)
    plane[3] = pass_on(0, 3, 0, 3)
    plane[1] = pass_on(0, 1, 1, 0)
    pairs = [to_pair(0, 0)]

    with scope("w_ready01"):
        pl.semaphore_wait(ready.at[0], 1)
        pl.semaphore_wait(ready.at[1], 1)
    pl.semaphore_signal(ready.at[2], inc=1, device_id=along(-8), device_id_type=MESH)
    pl.semaphore_signal(ready.at[3], inc=1, device_id=along(8), device_id_type=MESH)

    with scope("w_mixes"):
        everything(mixed.at[pl.ds(0, 15)], mix_recv.at[0]).wait()
    for b in range(16):
        piece[2 * b : 2 * b + 2, :] = mixed[b]
    xall[xh * 4 + r, j] = piece[...].astype(BF16)

    mine = xh * 4 + r

    def far_pass(k, slot, dz):
        at = xall.at[mine, lax.rem(j + 8 - k, 8)]
        to = xlate.at[slot - 3, mine] if slot in (3, 4, 5) else at
        return send(at, to, afar_send.at[0], afar_recv.at[slot - 1], along(dz))

    def near_forward(k):
        late = 1 if k in (3, 4, 5) else 0
        at = xlate.at[k - 3, mine] if late else xall.at[mine, lax.rem(j + 8 - k, 8)]
        for s, flip in NEAR:
            send(at, at, anear_send.at[late], anear_recv.at[late], along(steps[s], flip))

    afar = {}
    afar[2] = far_pass(0, 2, 8)
    afar[6] = far_pass(0, 6, -8)
    afar[1] = far_pass(0, 1, 4)
    afar[7] = far_pass(0, 7, -4)
    near_forward(0)

    def await_plane(*slots):
        for slot in slots:
            with scope(f"w_plane{slot}"):
                plane[slot].wait_recv()

    def await_far(*slots):
        for slot in slots:
            with scope(f"w_afar{slot}"):
                afar[slot].wait_recv()

    await_plane(2)
    plane[6] = pass_on(2, 6, 0, 1, low)
    pairs.append(to_pair(2, 2))
    await_plane(3)
    plane[8] = pass_on(3, 8, 0, 3, high)
    pairs.append(to_pair(3, 3))
    with scope("w_rnear"):
        everything(near_in, rnear_recv.at[0]).wait()
    total = part[r, xh].astype(F32)
    for n in range(7):
        total = total + near_in[n].astype(F32)
    row, col = iota((64, 64), 0), iota((64, 64), 1)
    spread = one_hot(col == (row & 3) * 16 + (row >> 3) * 2 + ((row >> 2) & 1))
    total = dot(spread, total.astype(BF16).reshape(64, 512), ((1,), (0,)))
    send_far[...] = total.astype(BF16).reshape(8, 8, 512)

    with scope("w_ready23"):
        pl.semaphore_wait(ready.at[2], 1)
        pl.semaphore_wait(ready.at[3], 1)
    rfar = {}

    def far_sums(*slots):
        for k in slots:
            rfar[k] = send(send_far.at[lax.rem(j + k, 8)], far_in.at[k], rfar_send.at[0], rfar_recv.at[0], along(4 * k))

    far_sums(4)
    await_far(1)
    near_forward(1)
    await_far(7)
    near_forward(7)
    await_far(2)
    await_far(6)
    afar[4] = far_pass(2 + 4 * c, 4, 8 - 16 * c)
    afar[3] = far_pass(2, 3, 4)
    afar[5] = far_pass(6, 5, -4)
    far_sums(3, 5, 2, 6, 1, 7)
    near_forward(2)
    near_forward(6)

    await_plane(1)
    plane[4] = pass_on(1, 4, 0, 1)
    plane[5] = pass_on(1, 5, 0, 3)
    pairs.append(to_pair(1, 1))

    await_plane(6)
    plane[7] = pass_on(6, 7, 1, 0, low)
    await_plane(8)
    plane[9] = pass_on(6, 9, 1, 0, high)
    pairs.append(to_pair(6, 6))

    await_far(3)
    near_forward(3)
    await_far(5)
    near_forward(5)
    await_far(4)
    near_forward(4)

    await_plane(4)
    pairs.append(to_pair(4, 4))
    await_plane(5)
    pairs.append(to_pair(5, 5))
    await_plane(7)
    pairs.append(to_pair(7, 7, low))
    await_plane(9)
    pairs.append(to_pair(7, 8, high))
    with scope("w_pairs"):
        everything(gall.at[pl.ds(0, 8)], pair_recv.at[0]).wait()

    row, col = iota((256, 256), 0), iota((256, 256), 1)
    regroup = one_hot(col == ((row >> 1) & 15) * 16 + (row >> 5) * 2 + (row & 1))

    def weights(half, cls):
        x = dot(xall[half * 4 + cls].reshape(256, 128), regroup, ((0,), (0,))).astype(BF16)
        g = gall[:, cls, half].reshape(256, 896)
        return dot(x, g, ((1,), (0,)))

    acc[...] = weights(xh, r)
    row, col = iota((32, 256), 0), iota((32, 256), 1)
    for half, cls, late in classes:
        pick = jnp.concatenate([one_hot(col == (row >> 1) * 16 + 2 * place + (row & 1)) for place in late], axis=0)
        rows = dot(pick, gall[:, cls, half].reshape(256, 896), ((1,), (0,))).astype(BF16)
        glate[:, half * 4 + cls] = rows.reshape(3, 32, 896)

    with scope("w_anear"):
        everything(xall.at[pl.ds(0, 7), pl.ds(0, 5)], anear_recv.at[0]).wait()
    with scope("c_weights"):
        total = acc[...]
        for half, cls, late in classes[1:]:
            total = total + weights(half, cls)
        acc[...] = total

    with scope("w_rfar"):
        everything(far_in.at[pl.ds(1, 7)], rfar_recv.at[0]).wait()
    latent = send_far[j].astype(F32)
    for k in range(1, 8):
        latent = latent + far_in[k].astype(F32)
    for i in range(2):
        for q in range(4):
            natural[i : i + 1, 512 * q : 512 * q + 512] = latent[4 * i + q : 4 * i + q + 1, :]

    def norm_back(incoming, unit, inverse, gain):
        scaled = gain[...].reshape(1, -1) * incoming
        mean = jnp.mean(scaled * unit, axis=-1, keepdims=True)
        return inverse * (scaled - unit * mean)

    q_unit, q_inv, q_normed = norm(ql, qg)
    kv_unit, kv_inv, kv_normed = norm(kvl, kvg)
    dql[...] = norm_back(natural[:, 0:1536], q_unit, q_inv, qg)
    dkvl[...] = norm_back(natural[:, 1536:2048], kv_unit, kv_inv, kvg)

    with scope("w_late"):
        everything(xlate.at[:, pl.ds(0, 7)], anear_recv.at[1]).wait()
    with scope("c_late"):
        total = acc[...]
        for n in range(3):
            total = total + dot(xlate[n].reshape(256, 128), glate[n].reshape(256, 896), ((0,), (0,)))
        dqup[...] = total[0:96, 0:384]
        dkvup[...] = total[96:128, 384:896]

    with scope("w_sends"):
        everything(mixed.at[pl.ds(0, 15)], mix_send.at[0]).wait()
        everything(gall.at[pl.ds(0, 7)], plane_send.at[0]).wait()
        everything(gall.at[pl.ds(0, 8)], pair_send.at[0]).wait()
        everything(near_in, rnear_send.at[0]).wait()
        everything(far_in.at[pl.ds(1, 7)], rfar_send.at[0]).wait()
        everything(xall.at[0, pl.ds(0, 7)], afar_send.at[0]).wait()
        everything(xall.at[pl.ds(0, 7), pl.ds(0, 5)], anear_send.at[0]).wait()
        everything(xlate.at[:, pl.ds(0, 7)], anear_send.at[1]).wait()


def write_kernel(a, b, w, v, dql, dkvl, dqup, dkvup, sem):
    copies = [
        pltpu.make_async_copy(src, dst, sem.at[n])
        for n, (src, dst) in enumerate([(w, dqup), (v, dkvup), (a, dql), (b, dkvl)])
    ]
    for copy in copies:
        copy.start()
    for copy in copies:
        copy.wait()


def body(query_latent, key_value_latent, query_gain, key_value_gain, q_up, kv_up, grad_q, grad_kv):
    dma = pltpu.SemaphoreType.DMA
    vmem = pltpu.VMEM
    hbm = pl.BlockSpec(memory_space=pltpu.HBM)
    shapes = (
        jax.ShapeDtypeStruct((2, 1536), F32),
        jax.ShapeDtypeStruct((2, 512), F32),
        jax.ShapeDtypeStruct((96, 384), F32),
        jax.ShapeDtypeStruct((32, 512), F32),
    )
    results = pl.pallas_call(
        kernel,
        name="mla_up_backward",
        out_shape=tuple(vmem(shape.shape, F32) for shape in shapes),
        in_specs=[hbm] * 8,
        out_specs=(pl.BlockSpec(memory_space=pltpu.VMEM),) * 4,
        scratch_shapes=[
            vmem((2, 1536), BF16), vmem((2, 512), BF16), vmem((1536,), F32), vmem((512,), F32),
            vmem((1536, 384), BF16), vmem((512, 512), BF16), vmem((128, 896), BF16),
            vmem((16, 2, 128), F32),
            vmem((16, 2, 128), F32),
            vmem((32, 128), F32),
            vmem((16, 4, 2, 16, 896), BF16),
            vmem((8, 8, 32, 128), BF16),
            vmem((3, 8, 32, 128), BF16),
            vmem((3, 8, 32, 896), BF16),
            vmem((4, 2, 4, 16, 512), BF16),
            vmem((7, 4, 16, 512), BF16),
            vmem((8, 8, 512), BF16),
            vmem((8, 8, 512), BF16),
            vmem((2, 2048), F32),
            vmem((128, 896), F32),
            dma((7,)), dma((1,)), dma((1,)), dma((1,)), dma((9,)), dma((1,)), dma((1,)),
            dma((1,)), dma((1,)), dma((1,)), dma((1,)), dma((1,)), dma((7,)), dma((2,)), dma((2,)),
            pltpu.SemaphoreType.REGULAR((4,)),
        ],
        compiler_params=pltpu.CompilerParams(
            collective_id=0, has_side_effects=True, vmem_limit_bytes=60 * 1000 * 1000),
    )(query_latent, key_value_latent, query_gain, key_value_gain, q_up, kv_up, grad_q, grad_kv)
    return pl.pallas_call(
        write_kernel,
        name="write_results",
        out_shape=shapes,
        in_specs=[pl.BlockSpec(memory_space=pltpu.VMEM)] * 4,
        out_specs=(hbm,) * 4,
        scratch_shapes=[dma((4,))],
        compiler_params=pltpu.CompilerParams(vmem_limit_bytes=1024 * 1024),
    )(*results)


def solution(mesh):
    group = ("dp", "tensor")
    placed = (
        P(group, None), P(group, None), P(), P(), P(None, "tensor"), P(None, "tensor"),
        P("dp", "tensor"), P("dp", "tensor"),
    )
    return jax.shard_map(
        body,
        mesh=mesh,
        in_specs=placed,
        out_specs=(P(group, None), P(group, None), P("dp", "tensor"), P("dp", "tensor")),
        check_vma=False,
    )
```
